32 devices in a mesh: dp: 8 (over z, core), tensor: 4 (over y, x).
Axes of the slice: x: 2, y: 2, z: 4, core: 2. Of those that a mesh axis runs over, the one named last changes fastest.
Arguments:
- tokens: bfloat16 [1024, 2048], P(('dp', 'tensor')), may hold values from -6 to 6
- gate_weight: bfloat16 [2048, 8192], P(None, 'tensor'), may hold values from -0.125 to 0.125
- up_act: bfloat16 [1024, 8192], P('dp', 'tensor'), may hold values from -6 to 6
- cotangent: bfloat16 [1024, 8192], P('dp', 'tensor'), may hold values from -6 to 6
- moment1: bfloat16 [2048, 8192], P('dp', 'tensor'), may hold values from -0.359375 to 0.359375
- moment2: bfloat16 [2048, 8192], P('dp', 'tensor'), may hold values from 0.0039978027 to 0.039794922
Outputs:
- in_grad: bfloat16 [1024, 2048], P(('dp', 'tensor'))
- up_grad: bfloat16 [1024, 8192], P('dp', 'tensor')
- new_moment1: bfloat16 [2048, 8192], P('dp', 'tensor')
- new_moment2: bfloat16 [2048, 8192], P('dp', 'tensor')
- update: float32 [2048, 8192], P('dp', 'tensor')
The draws below stay inside these ranges and needn't reach their ends.
All inputs are finite; a program needn't handle non-finite values.
Results may differ from the reference program's by a relative error of at most 0.015.
Values may be sent and summed in bfloat16 or wider, within the bound.
A program may use at most 64 MiB of HBM per device.

```python
import math
import jax
import jax.numpy as jnp
from jax import lax

DW = 2048
FFW = 8192
GROUP = 128
REPLICAS = 8
TENSOR_WAYS = 4
TOKENS = 1024


def strengthened(array, own_key, source, target, parts, factor):
    def block_of(axis_at):
        return (jnp.arange(array.shape[axis_at]) // (array.shape[axis_at] // parts)).reshape((-1,) + (1,) * (array.ndim - 1 - axis_at))

    one_side = jax.random.permutation(own_key, parts)[block_of(target)]
    second = (block_of(target) + parts // 2) % parts
    return jnp.where((block_of(source) == one_side) | (block_of(source) == second), factor * array, array)


def block_levels(rng, shape, cuts, smallest, high):
    def one(position, blocks):
        heights = jax.random.uniform(jax.random.fold_in(jax.random.fold_in(rng, 6), position), (blocks,), jnp.float32, smallest / len(cuts), high / len(cuts))
        return jnp.repeat(jnp.exp(heights), shape[position] // blocks).reshape((-1,) + (1,) * (len(shape) - position - 1))

    factor_of = one(*cuts[0])
    for cut in cuts[1:]:
        factor_of = factor_of * one(*cut)
    return factor_of


def gaussian(stream_key, dims, deviation, most, shards=(), dtype=jnp.bfloat16):
    drawn = jax.random.normal(stream_key, dims, jnp.float32) * deviation
    if len(shards) > 0:
        drawn = block_levels(stream_key, dims, shards, -0.22, 0.18) * drawn
    return jnp.clip(drawn, min=-most, max=most).astype(dtype)


def gaussian_with(stream_key, shape, deviation, bound, shards, heavy, held_as=jnp.bfloat16):
    values = deviation * jax.random.normal(stream_key, shape, jnp.float32)
    if shards:
        values = values * block_levels(stream_key, shape, shards, -0.22, 0.18)
    return jnp.clip(strengthened(values, jax.random.fold_in(stream_key, 3), *heavy), -bound, bound).astype(held_as)


def setup_inputs(seed: int = 0) -> dict:
    keys = jax.random.split(jax.random.key(seed), 7)
    tokens = gaussian_with(keys[0], (TOKENS, DW), 1.0, 6.0, ((0, 32),), (0, 1, 32, 2.75))
    gate_weight = gaussian(keys[1], (DW, FFW), DW ** -0.5, 0.125, ((1, 4),))
    up_act = gaussian(keys[2], (TOKENS, FFW), 1.0, 6.0, ((0, 8), (1, 4)))
    cotangent = gaussian(keys[3], (TOKENS, FFW), 1.0, 6.0, ((0, 8), (1, 4)))
    moment1 = gaussian(keys[4], (DW, FFW), 0.06, 0.359375, ((0, 8), (1, 4)))
    moment2 = jnp.clip(jnp.exp(math.log(0.039794922) - 2.2979944 * jax.random.uniform(keys[5], (DW, FFW), jnp.float32) ** block_levels(keys[5], (DW, FFW), ((0, 8), (1, 4)), -0.2, 0.2)), 0.0039978027, 0.039794922).astype(jnp.bfloat16)
    return dict(tokens=tokens, gate_weight=gate_weight, up_act=up_act, cotangent=cotangent, moment1=moment1, moment2=moment2)


def reference(tokens, gate_weight, up_act, cotangent, moment1, moment2):
    hidden_cols = FFW // TENSOR_WAYS
    token_sets = tokens.reshape(REPLICAS, GROUP, DW)
    up_sets = up_act.reshape(REPLICAS, GROUP, FFW)
    cot_sets = cotangent.reshape(REPLICAS, GROUP, FFW)
    weight_blocks = gate_weight.astype(jnp.float32).reshape(DW, TENSOR_WAYS, hidden_cols)

    def replica(running, operands):
        feature_rows, up_rows, cot_rows = operands
        gate_pre = jnp.dot(feature_rows, gate_weight, preferred_element_type=jnp.float32)
        sigmoid_gate = jax.nn.sigmoid(gate_pre)
        cot_float = cot_rows.astype(jnp.float32)
        up_result = (cot_float * gate_pre * sigmoid_gate).astype(jnp.bfloat16)
        gate_grad = (cot_float * up_rows.astype(jnp.float32) * sigmoid_gate * (1.0 + gate_pre * (1.0 - sigmoid_gate))).astype(jnp.bfloat16)
        pieces = jnp.einsum('gkc,dkc->kgd', gate_grad.astype(jnp.float32).reshape(GROUP, TENSOR_WAYS, hidden_cols), weight_blocks)
        input_rows = lax.optimization_barrier(jnp.sum(pieces.astype(jnp.bfloat16).astype(jnp.float32), axis=0)).astype(jnp.bfloat16)
        partial_value = jnp.dot(feature_rows.T, gate_grad, preferred_element_type=jnp.float32).astype(jnp.bfloat16)
        return (running + partial_value.astype(jnp.float32), (input_rows, up_result))
    start_sum = jnp.zeros((DW, FFW), jnp.float32)
    grad_total, (input_sets, up_results) = lax.scan(replica, start_sum, (token_sets, up_sets, cot_sets))
    grad = grad_total * (1.0 / math.sqrt(REPLICAS * GROUP))
    first = 0.9 * moment1.astype(jnp.float32) + 0.1 * grad
    second = 0.95 * moment2.astype(jnp.float32) + 0.05 * grad * grad
    update = first / (jnp.sqrt(second) + 1e-08)
    return (input_sets.reshape(TOKENS, DW), up_results.reshape(TOKENS, FFW), first.astype(jnp.bfloat16), second.astype(jnp.bfloat16), update)
```

```python
import functools
import math

import jax
import jax.numpy as jnp
from jax import lax
from jax.experimental import pallas as pl
from jax.experimental.pallas import tpu as pltpu
from jax.sharding import PartitionSpec as P

MESH = pl.DeviceIdType.MESH
F32, BF16 = jnp.float32, jnp.bfloat16
CORES = 2
WIDE = 256
VMEM_BUDGET = 60 * 2**20


def adam(grad, moment1, moment2):
    first = 0.9 * moment1.astype(F32) + 0.1 * grad
    second = 0.95 * moment2.astype(F32) + 0.05 * grad * grad
    return first, second, first / (jnp.sqrt(second) + 1e-08)


def activation_grads(gate_pre, cot, up):
    sig = jax.nn.sigmoid(gate_pre)
    cot = cot.astype(F32)
    up_grad = (cot * gate_pre * sig).astype(BF16)
    gate_grad = (cot * up.astype(F32) * sig * (1.0 + gate_pre * (1.0 - sig))).astype(BF16)
    return up_grad, gate_grad


def kernel(ndp, nt, tok, w, up, cot, m1, m2, in_grad, up_grad, nm1, nm2, upd,
           tg, xg, xt, wv, upv, cotv, m1v, m2v, gall, term, termr,
           loc_sem, w_sem, tg_s, tg_r, x1_s, x1_r, x2_s, x2_r,
           us, ur, ds, dr, ps, pr, qs, qr, ts, tr):
    d, t = lax.axis_index("dp"), lax.axis_index("tensor")
    z, core = d // CORES, d % CORES
    nz = ndp // CORES
    mate = d + 1 - 2 * core
    m, dw = tok.shape
    g, hid = up.shape
    rw = m1.shape[0]
    nc, _, hc = wv.shape
    scale = 1.0 / math.sqrt(ndp * g)

    def rdma(src, dst, s, r, dp, tn):
        return pltpu.make_async_remote_copy(
            src_ref=src, dst_ref=dst, send_sem=s, recv_sem=r, device_id=(dp, tn), device_id_type=MESH)

    mine = pl.ds(pl.multiple_of(t * m, m), m)
    loads = [
        pltpu.make_async_copy(tok, tg.at[mine], loc_sem.at[0]),
        pltpu.make_async_copy(tok.at[:, pl.ds(pl.multiple_of(d * rw, rw), rw)], xg.at[d, t], loc_sem.at[1]),
        pltpu.make_async_copy(cot, cotv, loc_sem.at[2]),
        pltpu.make_async_copy(up, upv, loc_sem.at[3]),
        pltpu.make_async_copy(m1, m1v, loc_sem.at[4]),
        pltpu.make_async_copy(m2, m2v, loc_sem.at[5]),
    ]

    def w_load(c):
        return pltpu.make_async_copy(w.at[:, pl.ds(pl.multiple_of(c * hc, hc), hc)], wv.at[c], w_sem.at[c])

    loads[0].start()
    loads[1].start()
    w_load(0).start()
    loads[2].start()
    loads[3].start()
    for c in range(1, nc):
        w_load(c).start()
    loads[4].start()
    loads[5].start()

    barrier = pltpu.get_barrier_semaphore()
    for k in range(1, nt):
        pl.semaphore_signal(barrier, inc=1, device_id=(d, lax.rem(t + k, nt)), device_id_type=MESH)
    for k in range(1, ndp):
        pl.semaphore_signal(barrier, inc=1, device_id=(lax.rem(d + k, ndp), t), device_id_type=MESH)
    loads[0].wait()
    loads[1].wait()
    pl.semaphore_wait(barrier, nt - 1 + ndp - 1)

    def tok_copy(k):
        return rdma(tg.at[mine], tg.at[mine], tg_s.at[k], tg_r.at[k], d, lax.rem(t + k, nt))

    def tok_recv(k):
        rows = pl.ds(pl.multiple_of(lax.rem(t + nt - k, nt) * m, m), m)
        return rdma(tg.at[rows], tg.at[rows], tg_s.at[k], tg_r.at[k], d, lax.rem(t + k, nt))

    def x1_copy(k):
        to = lax.rem(d + k, ndp)
        return rdma(tg.at[mine, pl.ds(pl.multiple_of(to * rw, rw), rw)], xg.at[d, t], x1_s.at[k], x1_r.at[k], to, t)

    def x1_recv(k):
        origin = lax.rem(d + ndp - k, ndp)
        return rdma(xg.at[origin, t], xg.at[origin, t], x1_s.at[k], x1_r.at[k], lax.rem(d + k, ndp), t)

    def x2_copy(k):
        return rdma(xg.at[:, t], xg.at[:, t], x2_s.at[k], x2_r.at[k], d, lax.rem(t + k, nt))

    def x2_recv(k):
        origin = lax.rem(t + nt - k, nt)
        return rdma(xg.at[:, origin], xg.at[:, origin], x2_s.at[k], x2_r.at[k], d, lax.rem(t + k, nt))

    for k in range(1, nt):
        tok_copy(k).start()
    for k in range(1, ndp):
        x1_copy(k).start()
    loads[2].wait()
    loads[3].wait()
    for k in range(1, nt):
        tok_recv(k).wait_recv()

    def block(c, chip, cr):
        return gall.at[c, pl.ds(pl.multiple_of((chip * CORES + cr) * g, g), g)]

    def up_copy(s, c):
        b = block(c, z - s, core)
        return rdma(b, b, us.at[s, c], ur.at[s, c], d + CORES, t)

    def down_copy(s, c):
        b = block(c, z + s, core)
        return rdma(b, b, ds.at[s, c], dr.at[s, c], d - CORES, t)

    def up_recv(s, c):
        b = block(c, z - s, core)
        return rdma(b, b, us.at[s - 1, c], ur.at[s - 1, c], d + CORES, t)

    def down_recv(s, c):
        b = block(c, z + s, core)
        return rdma(b, b, ds.at[s - 1, c], dr.at[s - 1, c], d - CORES, t)

    def mate_copy(s, c, low):
        b = block(c, z - s if low else z + s, core)
        return rdma(b, b, (ps if low else qs).at[s, c], (pr if low else qr).at[s, c], mate, t)

    def mate_recv(s, c, low):
        b = block(c, z - s if low else z + s, 1 - core)
        return rdma(b, b, (ps if low else qs).at[s, c], (pr if low else qr).at[s, c], mate, t)

    def hop(s, c):
        @pl.when(z - s >= 0)
        def _():
            if s > 0:
                up_recv(s, c).wait_recv()
            if s < nz - 1:
                @pl.when(z + 1 < nz)
                def _():
                    up_copy(s, c).start()
            mate_copy(s, c, True).start()

        @pl.when(z + s < nz)
        def _():
            if s > 0:
                down_recv(s, c).wait_recv()
            if s < nz - 1:
                @pl.when(z >= 1)
                def _():
                    down_copy(s, c).start()
            if s > 0:
                mate_copy(s, c, False).start()

    @pl.loop(0, nc)
    def _(c):
        w_load(c).wait()
        cols = pl.ds(pl.multiple_of(c * hc, hc), hc)
        gate_pre = jnp.dot(tg[...], wv[c], preferred_element_type=F32)
        ug, gg = activation_grads(gate_pre, cotv[:, cols], upv[:, cols])
        gall[c, pl.ds(pl.multiple_of(d * g, g), g), :] = gg
        up_grad[:, cols] = ug
        hop(0, c)

    for k in range(1, ndp):
        x1_recv(k).wait_recv()
    for k in range(1, nt):
        x2_copy(k).start()

    part = dw // nc

    @pl.loop(0, nc)
    def _(n):
        if nz > 1:
            hop(1, n)
        rows = pl.ds(pl.multiple_of(n * part, part), part)
        own = pl.ds(pl.multiple_of(d * g, g), g)
        total = jnp.zeros((g, part), F32)
        for c in range(nc):
            total += lax.dot_general(
                gall[c, own, :], wv[c, rows, :], (((1,), (1,)), ((), ())), preferred_element_type=F32)
        term[:, rows] = total.astype(BF16)

    for k in range(1, nt):
        x2_recv(k).wait_recv()
    for i in range(ndp):
        xt[:, i * g:(i + 1) * g] = xg[i].reshape(g, rw).T

    def term_copy(k):
        to = lax.rem(t + k, nt)
        return rdma(term.at[pl.ds(pl.multiple_of(to * m, m), m)], termr.at[k], ts.at[k], tr.at[k], d, to)

    for k in range(1, nt):
        term_copy(k).start()
    for s in range(2, nz - 1):
        @pl.loop(0, nc)
        def _(c):
            hop(s, c)
    total = term[mine, :].astype(F32)
    for k in range(1, nt):
        term_copy(k).wait_recv()
        total += termr[k].astype(F32)
    in_grad[...] = total.astype(BF16)
    loads[4].wait()
    loads[5].wait()

    @pl.loop(0, nc)
    def _(c):
        if nz > 2:
            hop(nz - 1, c)
        for s in range(nz):
            @pl.when(z - s >= 0)
            def _():
                mate_recv(s, c, True).wait_recv()
            if s > 0:
                @pl.when(z + s < nz)
                def _():
                    mate_recv(s, c, False).wait_recv()
        cols = pl.ds(pl.multiple_of(c * hc, hc), hc)
        grad = jnp.dot(xt[...], gall[c], preferred_element_type=F32) * scale
        first, second, step = adam(grad, m1v[:, cols], m2v[:, cols])
        nm1[:, cols] = first.astype(BF16)
        nm2[:, cols] = second.astype(BF16)
        upd[:, cols] = step

    for k in range(1, nt):
        tok_copy(k).wait_send()
        x2_copy(k).wait_send()
        term_copy(k).wait_send()
    for k in range(1, ndp):
        x1_copy(k).wait_send()

    @pl.loop(0, nc)
    def _(c):
        for s in range(nz):
            @pl.when(z - s >= 0)
            def _():
                mate_copy(s, c, True).wait_send()
                if s < nz - 1:
                    @pl.when(z + 1 < nz)
                    def _():
                        up_copy(s, c).wait_send()

            @pl.when(z + s < nz)
            def _():
                if s > 0:
                    mate_copy(s, c, False).wait_send()
                if s < nz - 1:
                    @pl.when(z >= 1)
                    def _():
                        down_copy(s, c).wait_send()


def fused(ndp, nt, tokens, gate_weight, up_act, cotangent, moment1, moment2):
    m, dw = tokens.shape
    g, hid = up_act.shape
    rw = moment1.shape[0]
    nc, nz = hid // WIDE, ndp // CORES
    any_spec, vmem = pl.BlockSpec(memory_space=pl.ANY), pl.BlockSpec(memory_space=pltpu.VMEM)
    dma = pltpu.SemaphoreType.DMA
    return pl.pallas_call(
        functools.partial(kernel, ndp, nt),
        out_shape=(
            jax.ShapeDtypeStruct((m, dw), BF16),
            jax.ShapeDtypeStruct((g, hid), BF16),
            jax.ShapeDtypeStruct((rw, hid), BF16),
            jax.ShapeDtypeStruct((rw, hid), BF16),
            jax.ShapeDtypeStruct((rw, hid), F32),
        ),
        in_specs=[any_spec] * 6,
        out_specs=(vmem,) * 5,
        scratch_shapes=[
            pltpu.VMEM((g, dw), BF16),
            pltpu.VMEM((ndp, nt, m, rw), BF16),
            pltpu.VMEM((rw, ndp * g), BF16),
            pltpu.VMEM((nc, dw, WIDE), BF16),
            pltpu.VMEM((g, hid), BF16),
            pltpu.VMEM((g, hid), BF16),
            pltpu.VMEM((rw, hid), BF16),
            pltpu.VMEM((rw, hid), BF16),
            pltpu.VMEM((nc, ndp * g, WIDE), BF16),
            pltpu.VMEM((g, dw), BF16),
            pltpu.VMEM((nt, m, dw), BF16),
            dma((6,)), dma((nc,)),
            dma((nt,)), dma((nt,)),
            dma((ndp,)), dma((ndp,)),
            dma((nt,)), dma((nt,)),
            dma((nz, nc)), dma((nz, nc)), dma((nz, nc)), dma((nz, nc)),
            dma((nz, nc)), dma((nz, nc)), dma((nz, nc)), dma((nz, nc)),
            dma((nt,)), dma((nt,)),
        ],
        compiler_params=pltpu.CompilerParams(
            collective_id=0, has_side_effects=True, vmem_limit_bytes=VMEM_BUDGET),
    )(tokens, gate_weight, up_act, cotangent, moment1, moment2)


def plain(ndp, nt, tokens, gate_weight, up_act, cotangent, moment1, moment2):
    gathered = lax.all_gather(tokens, "tensor", axis=0, tiled=True)
    gate_pre = jnp.dot(gathered, gate_weight, preferred_element_type=F32)
    up_grad, gate_grad = activation_grads(gate_pre, cotangent, up_act)
    term = lax.dot_general(
        gate_grad, gate_weight, (((1,), (1,)), ((), ())), preferred_element_type=F32).astype(BF16)
    in_grad = lax.psum_scatter(term, "tensor", scatter_dimension=0, tiled=True)
    partial_value = lax.dot_general(
        gathered, gate_grad, (((0,), (0,)), ((), ())), preferred_element_type=F32).astype(BF16)
    shard = lax.psum_scatter(partial_value.astype(F32), "dp", scatter_dimension=0, tiled=True)
    first, second, update = adam(shard * (1.0 / math.sqrt(ndp * gathered.shape[0])), moment1, moment2)
    return in_grad, up_grad, first.astype(BF16), second.astype(BF16), update


def local(ndp, nt, *args):
    (m, dw), (g, hid), rw = args[0].shape, args[2].shape, args[4].shape[0]
    need = (2 * dw * hid + 2 * ndp * g * (hid + 2 * rw) + 12 * g * hid + 16 * rw * hid + 16 * g * dw)
    fits = (need <= VMEM_BUDGET and ndp % CORES == 0 and ndp > CORES and nt > 1 and hid % WIDE == 0
            and g % 128 == 0 and rw % 128 == 0 and m % 16 == 0 and dw % (128 * (hid // WIDE)) == 0)
    return (fused if fits else plain)(ndp, nt, *args)


def solution(mesh):
    both = P("dp", "tensor")
    rows = P(("dp", "tensor"), None)
    return jax.shard_map(
        functools.partial(local, mesh.shape["dp"], mesh.shape["tensor"]),
        mesh=mesh,
        in_specs=(rows, P(None, "tensor"), both, both, both, both),
        out_specs=(rows, both, both, both, both),
        check_vma=False,
    )
```

```python
import functools
import math

import jax
import jax.numpy as jnp
from jax import lax
from jax.experimental import pallas as pl
from jax.experimental.pallas import tpu as pltpu
from jax.sharding import PartitionSpec as P

MESH = pl.DeviceIdType.MESH
F32, BF16 = jnp.float32, jnp.bfloat16
CORES = 2
WIDE = 256
VMEM_BUDGET = 48 * 2**20


def adam(grad, moment1, moment2):
    first = 0.9 * moment1.astype(F32) + 0.1 * grad
    second = 0.95 * moment2.astype(F32) + 0.05 * grad * grad
    return first, second, first / (jnp.sqrt(second) + 1e-08)


def activation_grads(gate_pre, cot, up):
    sig = jax.nn.sigmoid(gate_pre)
    cot = cot.astype(F32)
    up_grad = (cot * gate_pre * sig).astype(BF16)
    gate_grad = (cot * up.astype(F32) * sig * (1.0 + gate_pre * (1.0 - sig))).astype(BF16)
    return up_grad, gate_grad


def kernel(ndp, nt, tok, w, up, cot, m1, m2, in_grad, up_grad, nm1, nm2, upd,
           tg, xg, xt, wv, upv, cotv, m1v, m2v, gall, term, termr,
           loc_sem, w_sem, tg_s, tg_r, x1_s, x1_r, x2_s, x2_r,
           us, ur, ds, dr, ps, pr, qs, qr, ts, tr):
    d, t = lax.axis_index("dp"), lax.axis_index("tensor")
    z, core = d // CORES, d % CORES
    nz = ndp // CORES
    mate = d + 1 - 2 * core
    m, dw = tok.shape
    g, hid = up.shape
    rw = m1.shape[0]
    nc, _, hc = wv.shape
    scale = 1.0 / math.sqrt(ndp * g)

    def rdma(src, dst, s, r, dp, tn):
        return pltpu.make_async_remote_copy(
            src_ref=src, dst_ref=dst, send_sem=s, recv_sem=r, device_id=(dp, tn), device_id_type=MESH)

    mine = pl.ds(pl.multiple_of(t * m, m), m)
    loads = [
        pltpu.make_async_copy(tok, tg.at[mine], loc_sem.at[0]),
        pltpu.make_async_copy(tok.at[:, pl.ds(pl.multiple_of(d * rw, rw), rw)], xg.at[d, t], loc_sem.at[1]),
        pltpu.make_async_copy(cot, cotv, loc_sem.at[2]),
        pltpu.make_async_copy(up, upv, loc_sem.at[3]),
        pltpu.make_async_copy(m1, m1v, loc_sem.at[4]),
        pltpu.make_async_copy(m2, m2v, loc_sem.at[5]),
    ]

    def w_load(c):
        return pltpu.make_async_copy(w.at[:, pl.ds(pl.multiple_of(c * hc, hc), hc)], wv.at[c], w_sem.at[c])

    loads[0].start()
    loads[1].start()
    w_load(0).start()
    loads[2].start()
    loads[3].start()
    for c in range(1, nc):
        w_load(c).start()
    loads[4].start()
    loads[5].start()

    barrier = pltpu.get_barrier_semaphore()
    for k in range(1, nt):
        pl.semaphore_signal(barrier, inc=1, device_id=(d, lax.rem(t + k, nt)), device_id_type=MESH)
    for k in range(1, ndp):
        pl.semaphore_signal(barrier, inc=1, device_id=(lax.rem(d + k, ndp), t), device_id_type=MESH)
    loads[0].wait()
    loads[1].wait()
    pl.semaphore_wait(barrier, nt - 1 + ndp - 1)

    def tok_copy(k):
        return rdma(tg.at[mine], tg.at[mine], tg_s.at[k], tg_r.at[k], d, lax.rem(t + k, nt))

    def tok_recv(k):
        rows = pl.ds(pl.multiple_of(lax.rem(t + nt - k, nt) * m, m), m)
        return rdma(tg.at[rows], tg.at[rows], tg_s.at[k], tg_r.at[k], d, lax.rem(t + k, nt))

    def x1_copy(k):
        to = lax.rem(d + k, ndp)
        return rdma(tg.at[mine, pl.ds(pl.multiple_of(to * rw, rw), rw)], xg.at[d, t], x1_s.at[k], x1_r.at[k], to, t)

    def x1_recv(k):
        origin = lax.rem(d + ndp - k, ndp)
        return rdma(xg.at[origin, t], xg.at[origin, t], x1_s.at[k], x1_r.at[k], lax.rem(d + k, ndp), t)

    def x2_copy(k):
        return rdma(xg.at[:, t], xg.at[:, t], x2_s.at[k], x2_r.at[k], d, lax.rem(t + k, nt))

    def x2_recv(k):
        origin = lax.rem(t + nt - k, nt)
        return rdma(xg.at[:, origin], xg.at[:, origin], x2_s.at[k], x2_r.at[k], d, lax.rem(t + k, nt))

    for k in range(1, nt):
        tok_copy(k).start()
    for k in range(1, ndp):
        x1_copy(k).start()
    loads[2].wait()
    loads[3].wait()
    for k in range(1, nt):
        tok_recv(k).wait_recv()

    def block(c, chip, cr):
        return gall.at[c, pl.ds(pl.multiple_of((chip * CORES + cr) * g, g), g)]

    def up_copy(s, c):
        b = block(c, z - s, core)
        return rdma(b, b, us.at[s, c], ur.at[s, c], d + CORES, t)

    def down_copy(s, c):
        b = block(c, z + s, core)
        return rdma(b, b, ds.at[s, c], dr.at[s, c], d - CORES, t)

    def up_recv(s, c):
        b = block(c, z - s, core)
        return rdma(b, b, us.at[s - 1, c], ur.at[s - 1, c], d + CORES, t)

    def down_recv(s, c):
        b = block(c, z + s, core)
        return rdma(b, b, ds.at[s - 1, c], dr.at[s - 1, c], d - CORES, t)

    def mate_copy(s, c, low):
        b = block(c, z - s if low else z + s, core)
        return rdma(b, b, (ps if low else qs).at[s, c], (pr if low else qr).at[s, c], mate, t)

    def mate_recv(s, c, low):
        b = block(c, z - s if low else z + s, 1 - core)
        return rdma(b, b, (ps if low else qs).at[s, c], (pr if low else qr).at[s, c], mate, t)

    def hop(s, c):
        @pl.when(z - s >= 0)
        def _():
            if s > 0:
                up_recv(s, c).wait_recv()
            if s < nz - 1:
                @pl.when(z + 1 < nz)
                def _():
                    up_copy(s, c).start()
            mate_copy(s, c, True).start()

        @pl.when(z + s < nz)
        def _():
            if s > 0:
                down_recv(s, c).wait_recv()
            if s < nz - 1:
                @pl.when(z >= 1)
                def _():
                    down_copy(s, c).start()
            if s > 0:
                mate_copy(s, c, False).start()

    @pl.loop(0, nc)
    def _(c):
        w_load(c).wait()
        cols = pl.ds(pl.multiple_of(c * hc, hc), hc)
        gate_pre = jnp.dot(tg[...], wv[c], preferred_element_type=F32)
        ug, gg = activation_grads(gate_pre, cotv[:, cols], upv[:, cols])
        gall[c, pl.ds(pl.multiple_of(d * g, g), g), :] = gg
        up_grad[:, cols] = ug
        hop(0, c)

    for k in range(1, ndp):
        x1_recv(k).wait_recv()
    for k in range(1, nt):
        x2_copy(k).start()

    part = dw // nc

    @pl.loop(0, nc)
    def _(n):
        if nz > 1:
            hop(1, n)
        rows = pl.ds(pl.multiple_of(n * part, part), part)
        own = pl.ds(pl.multiple_of(d * g, g), g)
        total = jnp.zeros((g, part), F32)
        for c in range(nc):
            total += lax.dot_general(
                gall[c, own, :], wv[c, rows, :], (((1,), (1,)), ((), ())), preferred_element_type=F32)
        term[:, rows] = total.astype(BF16)

    for k in range(1, nt):
        x2_recv(k).wait_recv()
    for i in range(ndp):
        xt[:, i * g:(i + 1) * g] = xg[i].reshape(g, rw).T

    def term_copy(k):
        to = lax.rem(t + k, nt)
        return rdma(term.at[pl.ds(pl.multiple_of(to * m, m), m)], termr.at[k], ts.at[k], tr.at[k], d, to)

    for k in range(1, nt):
        term_copy(k).start()
    for s in range(2, nz - 1):
        @pl.loop(0, nc)
        def _(c):
            hop(s, c)
    total = term[mine, :].astype(F32)
    for k in range(1, nt):
        term_copy(k).wait_recv()
        total += termr[k].astype(F32)
    in_grad[...] = total.astype(BF16)
    loads[4].wait()
    loads[5].wait()

    @pl.loop(0, nc)
    def _(c):
        if nz > 2:
            hop(nz - 1, c)
        for s in range(nz):
            @pl.when(z - s >= 0)
            def _():
                mate_recv(s, c, True).wait_recv()
            if s > 0:
                @pl.when(z + s < nz)
                def _():
                    mate_recv(s, c, False).wait_recv()
        cols = pl.ds(pl.multiple_of(c * hc, hc), hc)
        grad = jnp.dot(xt[...], gall[c], preferred_element_type=F32) * scale
        first, second, step = adam(grad, m1v[:, cols], m2v[:, cols])
        nm1[:, cols] = first.astype(BF16)
        nm2[:, cols] = second.astype(BF16)
        upd[:, cols] = step

    for k in range(1, nt):
        tok_copy(k).wait_send()
        x2_copy(k).wait_send()
        term_copy(k).wait_send()
    for k in range(1, ndp):
        x1_copy(k).wait_send()

    @pl.loop(0, nc)
    def _(c):
        for s in range(nz):
            @pl.when(z - s >= 0)
            def _():
                mate_copy(s, c, True).wait_send()
                if s < nz - 1:
                    @pl.when(z + 1 < nz)
                    def _():
                        up_copy(s, c).wait_send()

            @pl.when(z + s < nz)
            def _():
                if s > 0:
                    mate_copy(s, c, False).wait_send()
                if s < nz - 1:
                    @pl.when(z >= 1)
                    def _():
                        down_copy(s, c).wait_send()


def fused(ndp, nt, tokens, gate_weight, up_act, cotangent, moment1, moment2):
    m, dw = tokens.shape
    g, hid = up_act.shape
    rw = moment1.shape[0]
    nc, nz = hid // WIDE, ndp // CORES
    any_spec, vmem = pl.BlockSpec(memory_space=pltpu.HBM), pl.BlockSpec(memory_space=pltpu.VMEM)
    dma = pltpu.SemaphoreType.DMA
    results = (((m, dw), BF16), ((g, hid), BF16), ((rw, hid), BF16), ((rw, hid), BF16), ((rw, hid), F32))
    held = pl.pallas_call(
        functools.partial(kernel, ndp, nt),
        out_shape=tuple(pltpu.VMEM(shape, dtype) for shape, dtype in results),
        in_specs=[any_spec] * 6,
        out_specs=(vmem,) * 5,
        scratch_shapes=[
            pltpu.VMEM((g, dw), BF16),
            pltpu.VMEM((ndp, nt, m, rw), BF16),
            pltpu.VMEM((rw, ndp * g), BF16),
            pltpu.VMEM((nc, dw, WIDE), BF16),
            pltpu.VMEM((g, hid), BF16),
            pltpu.VMEM((g, hid), BF16),
            pltpu.VMEM((rw, hid), BF16),
            pltpu.VMEM((rw, hid), BF16),
            pltpu.VMEM((nc, ndp * g, WIDE), BF16),
            pltpu.VMEM((g, dw), BF16),
            pltpu.VMEM((nt, m, dw), BF16),
            dma((6,)), dma((nc,)),
            dma((nt,)), dma((nt,)),
            dma((ndp,)), dma((ndp,)),
            dma((nt,)), dma((nt,)),
            dma((nz, nc)), dma((nz, nc)), dma((nz, nc)), dma((nz, nc)),
            dma((nz, nc)), dma((nz, nc)), dma((nz, nc)), dma((nz, nc)),
            dma((nt,)), dma((nt,)),
        ],
        compiler_params=pltpu.CompilerParams(
            collective_id=0, has_side_effects=True, vmem_limit_bytes=VMEM_BUDGET),
    )(*(pltpu.with_memory_space_constraint(x, pltpu.HBM)
        for x in (tokens, gate_weight, up_act, cotangent, moment1, moment2)))
    return pl.pallas_call(
        write_out,
        out_shape=tuple(pltpu.HBM(shape, dtype) for shape, dtype in results),
        in_specs=[vmem] * 5,
        out_specs=(any_spec,) * 5,
        scratch_shapes=[dma((5,))],
        compiler_params=pltpu.CompilerParams(vmem_limit_bytes=2**20),
    )(*(pltpu.with_memory_space_constraint(x, pltpu.VMEM) for x in held))


def write_out(*refs):
    sems = refs[-1]
    copies = [pltpu.make_async_copy(refs[i], refs[5 + i], sems.at[i]) for i in range(5)]
    for copy in reversed(copies):
        copy.start()
    for copy in copies:
        copy.wait()


def plain(ndp, nt, tokens, gate_weight, up_act, cotangent, moment1, moment2):
    gathered = lax.all_gather(tokens, "tensor", axis=0, tiled=True)
    gate_pre = jnp.dot(gathered, gate_weight, preferred_element_type=F32)
    up_grad, gate_grad = activation_grads(gate_pre, cotangent, up_act)
    term = lax.dot_general(
        gate_grad, gate_weight, (((1,), (1,)), ((), ())), preferred_element_type=F32).astype(BF16)
    in_grad = lax.psum_scatter(term, "tensor", scatter_dimension=0, tiled=True)
    partial_value = lax.dot_general(
        gathered, gate_grad, (((0,), (0,)), ((), ())), preferred_element_type=F32).astype(BF16)
    shard = lax.psum_scatter(partial_value.astype(F32), "dp", scatter_dimension=0, tiled=True)
    first, second, update = adam(shard * (1.0 / math.sqrt(ndp * gathered.shape[0])), moment1, moment2)
    return in_grad, up_grad, first.astype(BF16), second.astype(BF16), update


def local(ndp, nt, *args):
    (m, dw), (g, hid), rw = args[0].shape, args[2].shape, args[4].shape[0]
    need = (2 * dw * hid + 2 * ndp * g * (hid + 2 * rw) + 12 * g * hid + 16 * rw * hid + 16 * g * dw)
    fits = (need <= VMEM_BUDGET and ndp % CORES == 0 and ndp > CORES and nt > 1 and hid % WIDE == 0
            and g % 128 == 0 and rw % 128 == 0 and m % 16 == 0 and dw % (128 * (hid // WIDE)) == 0)
    return (fused if fits else plain)(ndp, nt, *args)


def solution(mesh):
    both = P("dp", "tensor")
    rows = P(("dp", "tensor"), None)
    return jax.shard_map(
        functools.partial(local, mesh.shape["dp"], mesh.shape["tensor"]),
        mesh=mesh,
        in_specs=(rows, P(None, "tensor"), both, both, both, both),
        out_specs=(rows, both, both, both, both),
        check_vma=False,
    )
```

```python
import functools
import math

import jax
import jax.numpy as jnp
from jax import lax
from jax.experimental import pallas as pl
from jax.experimental.pallas import tpu as pltpu
from jax.sharding import PartitionSpec as P

MESH = pl.DeviceIdType.MESH
F32, BF16 = jnp.float32, jnp.bfloat16
CORES = 2
WIDE = 512
VMEM_BUDGET = 48 * 2**20


def adam(grad, moment1, moment2):
    first = 0.9 * moment1.astype(F32) + 0.1 * grad
    second = 0.95 * moment2.astype(F32) + 0.05 * grad * grad
    return first, second, first / (jnp.sqrt(second) + 1e-08)


def activation_grads(gate_pre, cot, up):
    sig = jax.nn.sigmoid(gate_pre)
    cot = cot.astype(F32)
    up_grad = (cot * gate_pre * sig).astype(BF16)
    gate_grad = (cot * up.astype(F32) * sig * (1.0 + gate_pre * (1.0 - sig))).astype(BF16)
    return up_grad, gate_grad


def kernel(ndp, nt, tok, w, up, cot, m1, m2, in_grad, up_grad, nm1, nm2, upd,
           tg, xg, xt, wv, upv, cotv, m1v, m2v, gall, term, termr,
           loc_sem, w_sem, tg_s, tg_r, x1_s, x1_r, x2_s, x2_r,
           us, ur, ds, dr, ps, pr, qs, qr, ts, tr):
    d, t = lax.axis_index("dp"), lax.axis_index("tensor")
    z, core = d // CORES, d % CORES
    nz = ndp // CORES
    mate = d + 1 - 2 * core
    m, dw = tok.shape
    g, hid = up.shape
    rw = m1.shape[0]
    nc, _, hc = wv.shape
    scale = 1.0 / math.sqrt(ndp * g)

    def rdma(src, dst, s, r, dp, tn):
        return pltpu.make_async_remote_copy(
            src_ref=src, dst_ref=dst, send_sem=s, recv_sem=r, device_id=(dp, tn), device_id_type=MESH)

    mine = pl.ds(pl.multiple_of(t * m, m), m)
    loads = [
        pltpu.make_async_copy(tok, tg.at[mine], loc_sem.at[0]),
        pltpu.make_async_copy(tok.at[:, pl.ds(pl.multiple_of(d * rw, rw), rw)], xg.at[d, t], loc_sem.at[1]),
        pltpu.make_async_copy(cot, cotv, loc_sem.at[2]),
        pltpu.make_async_copy(up, upv, loc_sem.at[3]),
        pltpu.make_async_copy(m1, m1v, loc_sem.at[4]),
        pltpu.make_async_copy(m2, m2v, loc_sem.at[5]),
    ]

    def w_load(c):
        return pltpu.make_async_copy(w.at[:, pl.ds(pl.multiple_of(c * hc, hc), hc)], wv.at[c], w_sem.at[c])

    loads[0].start()
    loads[1].start()
    w_load(0).start()
    loads[2].start()
    loads[3].start()
    for c in range(1, nc):
        w_load(c).start()
    loads[4].start()
    loads[5].start()

    barrier = pltpu.get_barrier_semaphore()
    for k in range(1, nt):
        pl.semaphore_signal(barrier, inc=1, device_id=(d, lax.rem(t + k, nt)), device_id_type=MESH)
    for k in range(1, ndp):
        pl.semaphore_signal(barrier, inc=1, device_id=(lax.rem(d + k, ndp), t), device_id_type=MESH)
    loads[0].wait()
    loads[1].wait()
    pl.semaphore_wait(barrier, nt - 1 + ndp - 1)

    def tok_copy(k):
        return rdma(tg.at[mine], tg.at[mine], tg_s.at[k], tg_r.at[k], d, lax.rem(t + k, nt))

    def tok_recv(k):
        rows = pl.ds(pl.multiple_of(lax.rem(t + nt - k, nt) * m, m), m)
        return rdma(tg.at[rows], tg.at[rows], tg_s.at[k], tg_r.at[k], d, lax.rem(t + k, nt))

    def x1_copy(k):
        to = lax.rem(d + k, ndp)
        return rdma(tg.at[mine, pl.ds(pl.multiple_of(to * rw, rw), rw)], xg.at[d, t], x1_s.at[k], x1_r.at[k], to, t)

    def x1_recv(k):
        origin = lax.rem(d + ndp - k, ndp)
        return rdma(xg.at[origin, t], xg.at[origin, t], x1_s.at[k], x1_r.at[k], lax.rem(d + k, ndp), t)

    def x2_copy(k):
        return rdma(xg.at[:, t], xg.at[:, t], x2_s.at[k], x2_r.at[k], d, lax.rem(t + k, nt))

    def x2_recv(k):
        origin = lax.rem(t + nt - k, nt)
        return rdma(xg.at[:, origin], xg.at[:, origin], x2_s.at[k], x2_r.at[k], d, lax.rem(t + k, nt))

    for k in range(1, nt):
        tok_copy(k).start()
    for k in range(1, ndp):
        x1_copy(k).start()
    loads[2].wait()
    loads[3].wait()
    for k in range(1, nt):
        tok_recv(k).wait_recv()

    def block(c, chip, cr):
        return gall.at[c, pl.ds(pl.multiple_of((chip * CORES + cr) * g, g), g)]

    def up_copy(s, c):
        b = block(c, z - s, core)
        return rdma(b, b, us.at[s, c], ur.at[s, c], d + CORES, t)

    def down_copy(s, c):
        b = block(c, z + s, core)
        return rdma(b, b, ds.at[s, c], dr.at[s, c], d - CORES, t)

    def up_recv(s, c):
        b = block(c, z - s, core)
        return rdma(b, b, us.at[s - 1, c], ur.at[s - 1, c], d + CORES, t)

    def down_recv(s, c):
        b = block(c, z + s, core)
        return rdma(b, b, ds.at[s - 1, c], dr.at[s - 1, c], d - CORES, t)

    def mate_copy(s, c, low):
        b = block(c, z - s if low else z + s, core)
        return rdma(b, b, (ps if low else qs).at[s, c], (pr if low else qr).at[s, c], mate, t)

    def mate_recv(s, c, low):
        b = block(c, z - s if low else z + s, 1 - core)
        return rdma(b, b, (ps if low else qs).at[s, c], (pr if low else qr).at[s, c], mate, t)

    def hop(s, c):
        @pl.when(z - s >= 0)
        def _():
            if s > 0:
                up_recv(s, c).wait_recv()
            if s < nz - 1:
                @pl.when(z + 1 < nz)
                def _():
                    up_copy(s, c).start()
            mate_copy(s, c, True).start()

        @pl.when(z + s < nz)
        def _():
            if s > 0:
                down_recv(s, c).wait_recv()
            if s < nz - 1:
                @pl.when(z >= 1)
                def _():
                    down_copy(s, c).start()
            if s > 0:
                mate_copy(s, c, False).start()

    @pl.loop(0, nc)
    def _(c):
        w_load(c).wait()
        cols = pl.ds(pl.multiple_of(c * hc, hc), hc)
        gate_pre = jnp.dot(tg[...], wv[c], preferred_element_type=F32)
        ug, gg = activation_grads(gate_pre, cotv[:, cols], upv[:, cols])
        gall[c, pl.ds(pl.multiple_of(d * g, g), g), :] = gg
        up_grad[:, cols] = ug
        hop(0, c)

    for k in range(1, ndp):
        x1_recv(k).wait_recv()
    for k in range(1, nt):
        x2_copy(k).start()

    part = dw // nc

    @pl.loop(0, nc)
    def _(n):
        if nz > 1:
            hop(1, n)
        rows = pl.ds(pl.multiple_of(n * part, part), part)
        own = pl.ds(pl.multiple_of(d * g, g), g)
        total = jnp.zeros((g, part), F32)
        for c in range(nc):
            total += lax.dot_general(
                gall[c, own, :], wv[c, rows, :], (((1,), (1,)), ((), ())), preferred_element_type=F32)
        term[:, rows] = total.astype(BF16)

    for k in range(1, nt):
        x2_recv(k).wait_recv()
    for i in range(ndp):
        xt[:, i * g:(i + 1) * g] = xg[i].reshape(g, rw).T

    def term_copy(k):
        to = lax.rem(t + k, nt)
        return rdma(term.at[pl.ds(pl.multiple_of(to * m, m), m)], termr.at[k], ts.at[k], tr.at[k], d, to)

    for k in range(1, nt):
        term_copy(k).start()
    for s in range(2, nz - 1):
        @pl.loop(0, nc)
        def _(c):
            hop(s, c)
    total = term[mine, :].astype(F32)
    for k in range(1, nt):
        term_copy(k).wait_recv()
        total += termr[k].astype(F32)
    in_grad[...] = total.astype(BF16)
    loads[4].wait()
    loads[5].wait()

    @pl.loop(0, nc)
    def _(c):
        if nz > 2:
            hop(nz - 1, c)
        for s in range(nz):
            @pl.when(z - s >= 0)
            def _():
                mate_recv(s, c, True).wait_recv()
            if s > 0:
                @pl.when(z + s < nz)
                def _():
                    mate_recv(s, c, False).wait_recv()
        cols = pl.ds(pl.multiple_of(c * hc, hc), hc)
        grad = jnp.dot(xt[...], gall[c], preferred_element_type=F32) * scale
        first, second, step = adam(grad, m1v[:, cols], m2v[:, cols])
        nm1[:, cols] = first.astype(BF16)
        nm2[:, cols] = second.astype(BF16)
        upd[:, cols] = step

    for k in range(1, nt):
        tok_copy(k).wait_send()
        x2_copy(k).wait_send()
        term_copy(k).wait_send()
    for k in range(1, ndp):
        x1_copy(k).wait_send()

    @pl.loop(0, nc)
    def _(c):
        for s in range(nz):
            @pl.when(z - s >= 0)
            def _():
                mate_copy(s, c, True).wait_send()
                if s < nz - 1:
                    @pl.when(z + 1 < nz)
                    def _():
                        up_copy(s, c).wait_send()

            @pl.when(z + s < nz)
            def _():
                if s > 0:
                    mate_copy(s, c, False).wait_send()
                if s < nz - 1:
                    @pl.when(z >= 1)
                    def _():
                        down_copy(s, c).wait_send()


def fused(ndp, nt, tokens, gate_weight, up_act, cotangent, moment1, moment2):
    m, dw = tokens.shape
    g, hid = up_act.shape
    rw = moment1.shape[0]
    nc, nz = hid // WIDE, ndp // CORES
    any_spec, vmem = pl.BlockSpec(memory_space=pltpu.HBM), pl.BlockSpec(memory_space=pltpu.VMEM)
    dma = pltpu.SemaphoreType.DMA
    results = (((m, dw), BF16), ((g, hid), BF16), ((rw, hid), BF16), ((rw, hid), BF16), ((rw, hid), F32))
    held = pl.pallas_call(
        functools.partial(kernel, ndp, nt),
        out_shape=tuple(pltpu.VMEM(shape, dtype) for shape, dtype in results),
        in_specs=[any_spec] * 6,
        out_specs=(vmem,) * 5,
        scratch_shapes=[
            pltpu.VMEM((g, dw), BF16),
            pltpu.VMEM((ndp, nt, m, rw), BF16),
            pltpu.VMEM((rw, ndp * g), BF16),
            pltpu.VMEM((nc, dw, WIDE), BF16),
            pltpu.VMEM((g, hid), BF16),
            pltpu.VMEM((g, hid), BF16),
            pltpu.VMEM((rw, hid), BF16),
            pltpu.VMEM((rw, hid), BF16),
            pltpu.VMEM((nc, ndp * g, WIDE), BF16),
            pltpu.VMEM((g, dw), BF16),
            pltpu.VMEM((nt, m, dw), BF16),
            dma((6,)), dma((nc,)),
            dma((nt,)), dma((nt,)),
            dma((ndp,)), dma((ndp,)),
            dma((nt,)), dma((nt,)),
            dma((nz, nc)), dma((nz, nc)), dma((nz, nc)), dma((nz, nc)),
            dma((nz, nc)), dma((nz, nc)), dma((nz, nc)), dma((nz, nc)),
            dma((nt,)), dma((nt,)),
        ],
        compiler_params=pltpu.CompilerParams(
            collective_id=0, has_side_effects=True, vmem_limit_bytes=VMEM_BUDGET),
    )(*(pltpu.with_memory_space_constraint(x, pltpu.HBM)
        for x in (tokens, gate_weight, up_act, cotangent, moment1, moment2)))
    return pl.pallas_call(
        write_out,
        out_shape=tuple(pltpu.HBM(shape, dtype) for shape, dtype in results),
        in_specs=[vmem] * 5,
        out_specs=(any_spec,) * 5,
        scratch_shapes=[dma((5,))],
        compiler_params=pltpu.CompilerParams(vmem_limit_bytes=2**20),
    )(*(pltpu.with_memory_space_constraint(x, pltpu.VMEM) for x in held))


def write_out(*refs):
    sems = refs[-1]
    copies = [pltpu.make_async_copy(refs[i], refs[5 + i], sems.at[i]) for i in range(5)]
    for copy in reversed(copies):
        copy.start()
    for copy in copies:
        copy.wait()


def plain(ndp, nt, tokens, gate_weight, up_act, cotangent, moment1, moment2):
    gathered = lax.all_gather(tokens, "tensor", axis=0, tiled=True)
    gate_pre = jnp.dot(gathered, gate_weight, preferred_element_type=F32)
    up_grad, gate_grad = activation_grads(gate_pre, cotangent, up_act)
    term = lax.dot_general(
        gate_grad, gate_weight, (((1,), (1,)), ((), ())), preferred_element_type=F32).astype(BF16)
    in_grad = lax.psum_scatter(term, "tensor", scatter_dimension=0, tiled=True)
    partial_value = lax.dot_general(
        gathered, gate_grad, (((0,), (0,)), ((), ())), preferred_element_type=F32).astype(BF16)
    shard = lax.psum_scatter(partial_value.astype(F32), "dp", scatter_dimension=0, tiled=True)
    first, second, update = adam(shard * (1.0 / math.sqrt(ndp * gathered.shape[0])), moment1, moment2)
    return in_grad, up_grad, first.astype(BF16), second.astype(BF16), update


def local(ndp, nt, *args):
    (m, dw), (g, hid), rw = args[0].shape, args[2].shape, args[4].shape[0]
    need = (2 * dw * hid + 2 * ndp * g * (hid + 2 * rw) + 12 * g * hid + 16 * rw * hid + 16 * g * dw)
    fits = (need <= VMEM_BUDGET and ndp % CORES == 0 and ndp > CORES and nt > 1 and hid % WIDE == 0
            and g % 128 == 0 and rw % 128 == 0 and m % 16 == 0 and dw % (128 * (hid // WIDE)) == 0)
    return (fused if fits else plain)(ndp, nt, *args)


def solution(mesh):
    both = P("dp", "tensor")
    rows = P(("dp", "tensor"), None)
    return jax.shard_map(
        functools.partial(local, mesh.shape["dp"], mesh.shape["tensor"]),
        mesh=mesh,
        in_specs=(rows, P(None, "tensor"), both, both, both, both),
        out_specs=(rows, both, both, both, both),
        check_vma=False,
    )
```
